8 devices in a mesh: rep: 2 (over y, z), dp: 4 (over x, core).
Axes of the slice: x: 2, y: 2, z: 1, core: 2. Of those that a mesh axis runs over, the one named last changes fastest.
Arguments:
- x: bfloat16 [8, 2048, 896], P(('rep', 'dp')), parts along dimension 0
- dy: bfloat16 [8, 2048, 896], P(('rep', 'dp')), parts along dimension 0
- w_gate: bfloat16 [2, 896, 3584], replicated
- w_up: bfloat16 [2, 896, 3584], replicated
- w_down: bfloat16 [2, 3584, 896], replicated
- m_w_gate: float32 [2, 896, 3584], P(None, 'dp')
- m_w_up: float32 [2, 896, 3584], P(None, 'dp')
- m_w_down: float32 [2, 3584, 896], P(None, 'dp')
- v_w_gate: float32 [2, 896, 3584], P(None, 'dp')
- v_w_up: float32 [2, 896, 3584], P(None, 'dp')
- v_w_down: float32 [2, 3584, 896], P(None, 'dp')
Outputs:
- output 1: bfloat16 [4, 896, 3584], P('rep'), parts along dimension 0
- output 2: bfloat16 [4, 896, 3584], P('rep'), parts along dimension 0
- output 3: bfloat16 [4, 3584, 896], P('rep'), parts along dimension 0
- output 4: float32 [4, 896, 3584], P('rep', 'dp'), parts along dimension 0
- output 5: float32 [4, 896, 3584], P('rep', 'dp'), parts along dimension 0
- output 6: float32 [4, 3584, 896], P('rep', 'dp'), parts along dimension 0
- output 7: float32 [4, 896, 3584], P('rep', 'dp'), parts along dimension 0
- output 8: float32 [4, 896, 3584], P('rep', 'dp'), parts along dimension 0
- output 9: float32 [4, 3584, 896], P('rep', 'dp'), parts along dimension 0
There are 2 independent parts. The reference program is written for one: setup_inputs(seed, part) draws one part's arguments, and reference() takes and returns one part's arrays. A program takes and returns all parts, laid end to end along the dimension named above; an argument that names none is the same for every part.
All inputs are finite; a program needn't handle non-finite values.
Results may differ from the reference program's by a relative error of at most 0.0246.
Values are sent between devices in bfloat16 or wider.
A program may use at most 2 GiB of HBM per device.

```python
import jax
import jax.numpy as jnp
from jax import lax

SEQUENCES = 4
TOKENS = 2048
D = 896
FF = 3584
LAYERS = 2
NAMES = ("w_gate", "w_up", "w_down")
SHAPES = {"w_gate": (LAYERS, D, FF), "w_up": (LAYERS, D, FF), "w_down": (LAYERS, FF, D)}


def bump(key, n, height):
    away = (jnp.arange(n, dtype=jnp.int32) - jax.random.randint(key, (), 0, n, jnp.int32)) % n
    return jnp.where(away < n // 8, height, 1.0)


def together(key, own, strength):
    shared = jax.random.normal(key, own.shape[1:], jnp.float32)
    return (own + strength * shared) * lax.rsqrt(1 + strength * strength)


def setup_inputs(seed: int = 0, part: int = 0) -> dict:
    kx, kdy, ka, kb, kz, kf, kh, kl, *keys = jax.random.split(jax.random.key(seed), 8 + 3 * len(NAMES))
    kx, kdy, ka, kb = (jax.random.fold_in(k, part) for k in (kx, kdy, ka, kb))
    kw, km, kv = (keys[i::3] for i in range(3))
    shape = (SEQUENCES, TOKENS, D)
    much_x, much_dy = jax.random.uniform(kz, (2,), jnp.float32, 0.0, 1.0)
    loud = 2.0 ** jax.random.uniform(jax.random.fold_in(kz, 1), (), jnp.float32, -1.0, 2.0)
    layers = 2.0 ** jax.random.uniform(kl, (LAYERS, 1, 1), jnp.float32, -1.0, 1.0)
    x = together(ka, jax.random.normal(kx, shape, jnp.float32), much_x) * bump(kf, D, 4.0)
    dy = together(kb, jax.random.normal(kdy, shape, jnp.float32), much_dy)
    drawn = {"x": x.astype(jnp.bfloat16), "dy": (loud * dy * (SEQUENCES * TOKENS) ** -0.5).astype(jnp.bfloat16)}
    for key, name in zip(kw, NAMES, strict=True):
        w = jax.random.normal(key, SHAPES[name], jnp.float32) * SHAPES[name][1] ** -0.5
        drawn[name] = (w * {"w_gate": 1.0, "w_up": bump(kh, FF, 4.0), "w_down": layers}[name]).astype(jnp.bfloat16)
    for key, name in zip(km, NAMES, strict=True):
        drawn[f"m_{name}"] = 0.1 * jax.random.normal(key, SHAPES[name], jnp.float32)
    for key, name in zip(kv, NAMES, strict=True):
        drawn[f"v_{name}"] = jax.random.uniform(key, SHAPES[name], jnp.float32, 0.005, 0.015)
    return drawn


def matmul(a, w):
    return jnp.dot(a, w, preferred_element_type=jnp.float32).astype(jnp.bfloat16)


def normed(h):
    wide = h.astype(jnp.float32)
    scale = lax.rsqrt(jnp.mean(wide**2, -1, keepdims=True) + 1e-6)
    return (wide * scale).astype(jnp.bfloat16)


def layer(h, w):
    a = normed(h)
    gate = jnp.dot(a, w["w_gate"], preferred_element_type=jnp.float32)
    up = jnp.dot(a, w["w_up"], preferred_element_type=jnp.float32)
    return h + matmul((jax.nn.silu(gate) * up).astype(jnp.bfloat16), w["w_down"])


def adamw(w, m, v, g):
    m = 0.9 * m + 0.1 * g
    v = 0.95 * v + 0.05 * g * g
    step = m * lax.rsqrt(v + 1e-8) + 0.1 * w
    return (w - 0.02 * step).astype(jnp.bfloat16), m, v


def stack(weights, h):
    return lax.scan(lambda h, w: (layer(h, w), None), h, weights)[0]


def reference(x, dy, w_gate, w_up, w_down, m_w_gate, m_w_up, m_w_down, v_w_gate, v_w_up, v_w_down):
    weights = dict(zip(NAMES, (w_gate, w_up, w_down), strict=True))

    def take(so_far, sequence):
        h, by_y = sequence
        _, back = jax.vjp(lambda w: stack(w, h), weights)
        return jax.tree.map(lambda total, term: total + term.astype(jnp.float32), so_far, back(by_y)[0]), None

    none_yet = {name: jnp.zeros(w.shape, jnp.float32) for name, w in weights.items()}
    by_weights, _ = lax.scan(take, none_yet, (x, dy))
    gradients = [by_weights[name].astype(jnp.bfloat16).astype(jnp.float32) for name in NAMES]
    new = [
        adamw(w.astype(jnp.float32), m, v, g)
        for w, m, v, g in zip((w_gate, w_up, w_down), (m_w_gate, m_w_up, m_w_down), (v_w_gate, v_w_up, v_w_down), gradients, strict=True)
    ]
    return tuple(one[which] for which in range(3) for one in new)
```

```python
import functools

import jax
import jax.numpy as jnp
from jax import lax
from jax.experimental import pallas as pl
from jax.experimental.pallas import tpu as pltpu
from jax.sharding import PartitionSpec as P

BF, F32 = jnp.bfloat16, jnp.float32
VMEM_LIMIT = 64 * 1024 * 1024 - 65536
BF_TILE = 256
LN = 128
OWN0 = 3


def dot(a, b):
    return jnp.dot(a, b, preferred_element_type=F32)


def dot_t(a, b):
    return lax.dot_general(a, b, (((1,), (1,)), ((), ())), preferred_element_type=F32)


def scale_of(wide):
    return lax.rsqrt(jnp.mean(wide**2, -1, keepdims=True) + 1e-6)


def normed(h):
    wide = h.astype(F32)
    return (wide * scale_of(wide)).astype(BF)


def rows_of(t, bm):
    return pl.ds(t * bm if isinstance(t, int) else pl.multiple_of(t * bm, bm), bm)


def skewed(nt, first, second, slots):
    first(0, slots[0])
    for t in range(1, nt):
        first(t, slots[t % 2])
        second(t - 1, slots[(t - 1) % 2])
    second(nt - 1, slots[(nt - 1) % 2])


def call(body, idx, grid, ins, outs, args, scratch=(), aliases=None, flops=0, nbytes=0, after=()):
    def spec(s):
        if s is None:
            return pl.BlockSpec(memory_space=pl.ANY)
        block, index, *single = s
        return pl.BlockSpec(block, index, **({"pipeline_mode": pl.Buffered(1)} if single else {}))

    n = len(args)

    def wrapped(idx, *refs):
        body(idx, *refs[:n], *refs[n + len(after) :])

    return pl.pallas_call(
        wrapped,
        grid_spec=pltpu.PrefetchScalarGridSpec(
            num_scalar_prefetch=1,
            grid=grid,
            in_specs=[spec(s) for s in list(ins) + [None] * len(after)],
            out_specs=[spec(s) for s, _ in outs],
            scratch_shapes=list(scratch),
        ),
        out_shape=[s for _, s in outs],
        input_output_aliases={k + 1: v for k, v in (aliases or {}).items()},
        compiler_params=pltpu.CompilerParams(vmem_limit_bytes=VMEM_LIMIT),
        cost_estimate=pl.CostEstimate(flops=flops, bytes_accessed=nbytes, transcendentals=0),
    )(idx, *args, *after)


def forward_body(nt, bm, n_alias, last, idx, x, wg, wu, wd, *rest):
    gate, up, h1, a0_t, a1, a1_t, a, acc, s0, s1 = rest[n_alias:]
    i = pl.program_id(0)

    @pl.when(i == 0)
    def _():
        def block(t, _):
            r = rows_of(t, bm)
            a[r, :] = normed(x[r, :])
            a0_t[:, r] = a[r, :].T
            acc[r, :] = jnp.zeros((bm, acc.shape[1]), F32)
            return 0

        lax.fori_loop(0, nt, block, 0)

    def first(t, s):
        r = rows_of(t, bm)
        g, u = dot(a[r, :], wg[...]), dot(a[r, :], wu[...])
        gate[r, :] = g
        up[r, :] = u
        s[...] = (jax.nn.silu(g) * u).astype(BF)

    def second(t, s):
        acc[rows_of(t, bm), :] += dot(s[...], wd[...])

    skewed(nt, first, second, (s0, s1))

    @pl.when(i == last)
    def _():
        def block(t, _):
            r = rows_of(t, bm)
            h1[r, :] = x[r, :] + acc[r, :].astype(BF)
            a1[r, :] = normed(h1[r, :])
            a1_t[:, r] = a1[r, :].T
            return 0

        lax.fori_loop(0, nt, block, 0)


def forward(idx, x, w, whole, start, bm, bufs, after=()):
    t, d = x.shape
    ff = w[0].shape[-1]
    n, at = ff // BF_TILE, start // t
    rows = ((t, d), lambda i, s: (at, 0), 1)
    columns = ((d, t), lambda i, s: (0, at), 1)
    tile = ((t, BF_TILE), lambda i, s: (at, i))
    outs = [
        (tile, jax.ShapeDtypeStruct((whole, ff), F32)),
        (tile, jax.ShapeDtypeStruct((whole, ff), F32)),
        (rows, jax.ShapeDtypeStruct((whole, d), BF)),
        (columns, jax.ShapeDtypeStruct((d, whole), BF)),
        (rows, jax.ShapeDtypeStruct((whole, d), BF)),
        (columns, jax.ShapeDtypeStruct((d, whole), BF)),
    ]
    n_alias = len(bufs)
    return call(
        functools.partial(forward_body, t // bm, bm, n_alias, n - 1),
        idx,
        (n,),
        [
            ((t, d), lambda i, s: (0, 0), 1),
            ((None, d, BF_TILE), lambda i, s: (0, 0, i)),
            ((None, d, BF_TILE), lambda i, s: (0, 0, i)),
            ((None, BF_TILE, d), lambda i, s: (0, i, 0)),
        ]
        + [None] * n_alias,
        outs,
        [x, *w, *bufs],
        scratch=[pltpu.VMEM((t, d), BF), pltpu.VMEM((t, d), F32)] + [pltpu.VMEM((bm, BF_TILE), BF)] * 2,
        aliases={4 + k: k for k in range(n_alias)},
        flops=6 * t * d * ff,
        nbytes=t * ff * 8 + 3 * d * ff * 2,
        after=after,
    )


def local_grads(g, u, dh):
    sg = jax.nn.sigmoid(g)
    act = g * sg
    return (act * u).astype(BF), (dh * u * (sg + act * (1 - sg))).astype(BF), (dh * act).astype(BF)


def pair(q0, q1, axis):
    return jnp.concatenate([q0[...], q1[...]], axis)


def hand_out(ci, acc_g, acc_u, keep, send):
    quarter = acc_g.shape[0] // 2
    for out, who in ((keep, ci), (send, 1 - ci)):
        for k, acc in enumerate((acc_g, acc_u)):
            block = acc[pl.ds(pl.multiple_of(who * quarter, quarter), quarter), :].astype(BF)
            for q in range(2):
                out[2 * k + q] = block[:, q * LN : (q + 1) * LN]


def hand_out_down(ci, acc_d, keep, send):
    for q in range(2):
        part = acc_d[:, q * LN : (q + 1) * LN].T.astype(BF)

        @pl.when(ci == q)
        def _():
            keep[...] = part

        @pl.when(ci != q)
        def _():
            send[...] = part


def middle_body(cfg, idx, *refs):
    nt, bm, parts_in, parts_out, whole, half = cfg
    refs = list(refs)
    take = lambda n: [refs.pop(0) for _ in range(n)]
    a_h, a_t_h, *dys_h = take(2 + (2 if whole else 1))
    wg, wu, wd = ((take(1)[0], take(1)[0]) for _ in range(3))
    parts = take(3 if parts_in else 0)
    das, h1_h = (take(2), take(1)[0]) if whole else ((), None)
    if parts_out:
        p_g, p_u, p_d = take(3)
    else:
        keep, send = take(2)
        keep_d, send_d = (None, None) if whole else take(2)
    result = take(1)[0]
    a, a_t, dy, da = take(4)
    dy_t, acc_d = (None, None) if whole else take(2)
    hbuf = take(1)[0] if whole else None
    acc_g, acc_u, s0, s1, sems = take(5)
    i, last = pl.program_id(0), pl.num_programs(0) - 1
    at = half * (nt * bm)
    r_own = a_t.shape[0]
    xi, ci = idx[0], idx[1]

    def copies(t, static):
        r = rows_of(t, bm)
        src = pl.ds(at + t * bm if static else pl.multiple_of(at + t * bm, bm), bm)
        own = pl.ds(pl.multiple_of(xi * r_own, r_own), r_own)
        if whole:
            per = nt // 2
            which, local = (t // per, rows_of(t % per, bm)) if static else (0, rows_of(0, bm))
            dy_src = dys_h[which].at[local, :]
            da_src = [das[which].at[local, :]]
        else:
            dy_src, da_src = dys_h[0].at[r, :], []
        yield pltpu.make_async_copy(a_h.at[src, :], a.at[r, :], sems.at[0, t])
        yield pltpu.make_async_copy(dy_src, dy.at[r, :], sems.at[1, t])
        yield pltpu.make_async_copy(a_t_h.at[own, src], a_t.at[:, r], sems.at[2, t])
        for d in da_src:
            yield pltpu.make_async_copy(d, da.at[r, :], sems.at[3, t])

    def first(t, s):
        r = rows_of(t, bm)
        g, u = dot(a[r, :], pair(*wg, 1)), dot(a[r, :], pair(*wu, 1))
        dh = dot_t(dy[r, :], pair(*wd, 0))
        s[2], s[0], s[1] = local_grads(g, u, dh.astype(BF).astype(F32))

    def second(t, s):
        r = rows_of(t, bm)
        da[r, :] += dot_t(s[0], pair(*wg, 1)) + dot_t(s[1], pair(*wu, 1))
        acc_g[...] += dot(a_t[:, r], s[0])
        acc_u[...] += dot(a_t[:, r], s[1])
        if not whole:
            acc_d[...] += dot(dy_t[:, r], s[2])

    if parts_in:
        acc_g[...], acc_u[...], acc_d[...] = (p[...] for p in parts)
    else:
        acc_g[...] = jnp.zeros_like(acc_g)
        acc_u[...] = jnp.zeros_like(acc_u)
        if not whole:
            acc_d[...] = jnp.zeros_like(acc_d)

    @pl.when(i == 0)
    def _():
        for t in range(nt):
            for c in copies(t, True):
                c.start()
        if not whole:
            da[...] = jnp.zeros_like(da)

        def block(t, _):
            for c in copies(t, False):
                c.wait()
            if not whole:
                dy_t[:, rows_of(t, bm)] = dy[rows_of(t, bm), :].T
            first(t, s0)
            second(t, s0)
            return 0

        lax.fori_loop(0, nt, block, 0)

    @pl.when(i > 0)
    def _():
        skewed(nt, first, second, (s0, s1))

    if parts_out:
        p_g[...], p_u[...], p_d[...] = acc_g[...], acc_u[...], acc_d[...]
    else:
        hand_out(ci, acc_g, acc_u, keep, send)
        if not whole:
            hand_out_down(ci, acc_d, keep_d, send_d)

    @pl.when(i == last)
    def _():
        bk = hbuf.shape[1] if whole else bm
        nk = nt * bm // bk

        def h_copy(k):
            return pltpu.make_async_copy(h1_h.at[rows_of(k, bk), :], hbuf.at[k % 2], sems.at[0, k % 2])

        def out_copy(k):
            src = dy if whole else da
            return pltpu.make_async_copy(src.at[rows_of(k, bk), :], result.at[rows_of(k, bk), :], sems.at[1, k])

        if whole:
            h_copy(0).start()

        def block(k, _):
            if whole:
                h_copy(k).wait()

                @pl.when(k + 1 < nk)
                def _():
                    h_copy(k + 1).start()

                r = rows_of(k, bk)
                wide = hbuf[k % 2].astype(F32)
                scale = scale_of(wide)
                ct = da[r, :].astype(BF).astype(F32)
                hat = wide * scale
                back = scale * (ct - hat * jnp.mean(ct * hat, -1, keepdims=True))
                dy[r, :] = dy[r, :] + back.astype(BF)
            out_copy(k).start()
            return 0

        lax.fori_loop(0, nk, block, 0)
        lax.fori_loop(0, nk, lambda k, _: (out_copy(k).wait(), 0)[1], 0)


def tile_specs(layer, base, d):
    q = lambda k: lambda s: base(s) * 2 + k
    columns = [((None, d, LN), lambda i, s, k=k: (layer, 0, base(s, k) + i)) for k in range(2)]
    rows = [((None, LN, d), lambda i, s, k=k: (layer, base(s, k) + i, 0)) for k in range(2)]
    return columns, rows


def grad_outs(r, d, n, with_d):
    gu = (((4, r // 2, LN), lambda i, s: (0, 0, i)), jax.ShapeDtypeStruct((4, r // 2, n * LN), BF))
    down = (((LN, d), lambda i, s: (i, 0)), jax.ShapeDtypeStruct((n * LN, d), BF))
    return [gu, gu] + ([down, down] if with_d else [])


def middle(idx, half, a, a_t, dys, w, n, base, parts=(), das=(), h1=None, parts_out=False, bm=1024, after=()):
    whole = len(das) > 0
    d, r = a.shape[1], a.shape[1] // 2
    t = dys[0].shape[0] * len(dys)
    nt = t // bm
    columns, rows = tile_specs(1, base, d)
    tile = lambda s: (s, lambda i, s: (0, i))
    ins = [None] * (2 + len(dys)) + columns + columns + rows
    args = [a, a_t, *dys, w[0], w[0], w[1], w[1], w[2], w[2]]
    part = [tile((r, 2 * LN)), tile((r, 2 * LN)), tile((d, 2 * LN))]
    if parts:
        ins += part
        args += parts
    if whole:
        ins += [None] * 3
        args += [*das, h1]
    if parts_out:
        outs = [(p, jax.ShapeDtypeStruct((p[0][0], n * 2 * LN), F32)) for p in part]
    else:
        outs = grad_outs(r, d, n, not whole)
    outs.append((None, jax.ShapeDtypeStruct((t, d), BF if whole else F32)))
    scratch = [pltpu.VMEM((t, d), BF), pltpu.VMEM((r, t), BF), pltpu.VMEM((t, d), BF), pltpu.VMEM((t, d), F32)]
    scratch += [pltpu.VMEM((2, 512, d), BF)] if whole else [pltpu.VMEM((d, t), BF), pltpu.VMEM((d, 2 * LN), F32)]
    scratch += [pltpu.VMEM((r, 2 * LN), F32)] * 2 + [pltpu.VMEM((3, bm, 2 * LN), BF)] * 2
    scratch += [pltpu.SemaphoreType.DMA((4, 8))]
    return call(
        functools.partial(middle_body, (nt, bm, bool(parts), parts_out, whole, half)),
        idx,
        (n,),
        ins,
        outs,
        args,
        scratch=scratch,
        flops=(12 if whole else 14) * t * d * n * 2 * LN,
        nbytes=t * d * 8 + 3 * d * n * 2 * LN * 2,
        after=after,
    )


def backward_body(nt, bm, with_d, idx, dh_h, a_t_h, *refs):
    refs = list(refs)
    take = lambda n: [refs.pop(0) for _ in range(n)]
    gate, up, wd = take(2), take(2), take(2)
    keep, send = take(2)
    keep_d, send_d = take(2) if with_d else (None, None)
    dh, a_t = take(2)
    dh_t, acc_d = take(2) if with_d else (None, None)
    acc_g, acc_u, s0, s1, sems = take(5)
    i = pl.program_id(0)
    r_own = a_t.shape[0]
    xi, ci = idx[0], idx[1]

    def copies(t):
        r = rows_of(t, bm)
        own = pl.ds(pl.multiple_of(xi * r_own, r_own), r_own)
        yield pltpu.make_async_copy(dh_h.at[r, :], dh.at[r, :], sems.at[0, t])
        yield pltpu.make_async_copy(a_t_h.at[own, r], a_t.at[:, r], sems.at[1, t])

    def first(t, s):
        r = rows_of(t, bm)
        dhid = dot_t(dh[r, :], pair(*wd, 0)).astype(BF).astype(F32)
        g, u = (jnp.concatenate([p[0][r, :], p[1][r, :]], 1) for p in (gate, up))
        s[2], s[0], s[1] = local_grads(g, u, dhid)

    def second(t, s):
        r = rows_of(t, bm)
        acc_g[...] += dot(a_t[:, r], s[0])
        acc_u[...] += dot(a_t[:, r], s[1])
        if with_d:
            acc_d[...] += dot(dh_t[:, r], s[2])

    acc_g[...] = jnp.zeros_like(acc_g)
    acc_u[...] = jnp.zeros_like(acc_u)
    if with_d:
        acc_d[...] = jnp.zeros_like(acc_d)

    @pl.when(i == 0)
    def _():
        for t in range(nt):
            for c in copies(t):
                c.start()

        def block(t, _):
            for c in copies(t):
                c.wait()
            if with_d:
                dh_t[:, rows_of(t, bm)] = dh[rows_of(t, bm), :].T
            first(t, s0)
            second(t, s0)
            return 0

        lax.fori_loop(0, nt, block, 0)

    @pl.when(i > 0)
    def _():
        skewed(nt, first, second, (s0, s1))

    hand_out(ci, acc_g, acc_u, keep, send)
    if with_d:
        hand_out_down(ci, acc_d, keep_d, send_d)


def backward(idx, dh, a_t, gate, up, wd, n, base, with_d, bm=1024, after=()):
    t, d = dh.shape
    r = d // 2
    _, rows = tile_specs(0, base, d)
    acts = [((t, LN), lambda i, s, k=k: (0, base(s, k) + i)) for k in range(2)]
    return call(
        functools.partial(backward_body, t // bm, bm, with_d),
        idx,
        (n,),
        [None, None] + acts + acts + rows,
        grad_outs(r, d, n, with_d),
        [dh, a_t, gate, gate, up, up, wd, wd],
        scratch=[pltpu.VMEM((t, d), BF), pltpu.VMEM((r, t), BF)]
        + ([pltpu.VMEM((d, t), BF), pltpu.VMEM((d, 2 * LN), F32)] if with_d else [])
        + [pltpu.VMEM((r, 2 * LN), F32)] * 2
        + [pltpu.VMEM((3, bm, 2 * LN), BF)] * 2
        + [pltpu.SemaphoreType.DMA((2, 8))],
        flops=(5 if with_d else 4) * t * d * n * 2 * LN,
        nbytes=t * n * 2 * LN * 8,
        after=after,
    )


def places(layer, own, first, n, quarter, part, px, pc):
    base = (px if own else 1 - px) * 2 * part + first * LN
    al = lambda v: pl.multiple_of(v, LN)
    gu = [
        (k, (layer, pl.ds((2 * px + pc) * quarter, quarter), pl.ds(al(base + q * part), n * LN))) for k in range(2) for q in range(2)
    ]
    return gu, (layer, pl.ds(al((2 * px + pc) * part + first * LN), n * LN), slice(None))


def adam_body(layer, own, first, n, n_bufs, idx, *refs):
    refs = list(refs)
    take = lambda n: [refs.pop(0) for _ in range(n)]
    jobs_n = 5 if own else 4
    kinds = 3 if own else 2
    mine, theirs = take(kinds - 1), take(kinds - 1)
    w, m, v = take(kinds), take(kinds), take(kinds)
    take(n_bufs)
    w_new, m_new, v_new = take(kinds), take(kinds), take(kinds)
    pieces = take(kinds - 1)
    scratch = take(2 * 7 if own else 7)
    sem_in, sem_out = take(2)
    quarter, part = m[0].shape[1], m[0].shape[2] // 4
    xi, ci = idx[0], idx[1]
    gu, down = places(layer, own, first, n, quarter, part, xi, ci)
    jobs = []
    for j, (k, at) in enumerate(gu):
        local = (layer, slice(None), at[2])
        jobs.append((j, k, at, local, lambda r, j=j: r[0].at[j], [s.at[j] for s in scratch[:7]]))
    if own:
        local = (layer, pl.ds(first * LN, n * LN), slice(None))
        jobs.append((4, 2, down, local, lambda r: r[1], scratch[7:]))
    ins = []
    for j, k, at, local, of, (g0, g1, ws, ms, vs, *_) in jobs:
        src = [of(mine), of(theirs), w[k].at[at], m[k].at[local], v[k].at[local]]
        ins.append([pltpu.make_async_copy(s, d, sem_in.at[j, p]) for p, (s, d) in enumerate(zip(src, (g0, g1, ws, ms, vs)))])
        for c in ins[-1]:
            c.start()
    outs = []
    for (j, k, at, local, of, (g0, g1, ws, ms, vs, mo, vo)), cs in zip(jobs, ins):
        for c in cs:
            c.wait()
        rows = g0.shape[0]
        step = 32

        def block(b, _, g0=g0, g1=g1, ws=ws, ms=ms, vs=vs, mo=mo, vo=vo):
            r = rows_of(b, step)
            g = (g0[r, :].astype(F32) + g1[r, :].astype(F32)).astype(BF).astype(F32)
            mm = 0.9 * ms[r, :] + 0.1 * g
            vv = 0.95 * vs[r, :] + 0.05 * g * g
            wide = ws[r, :].astype(F32)
            ws[r, :] = (wide - 0.02 * (mm * lax.rsqrt(vv + 1e-8) + 0.1 * wide)).astype(BF)
            mo[r, :] = mm
            vo[r, :] = vv
            return 0

        lax.fori_loop(0, rows // step, block, 0)
        pairs = [(ws, of(pieces)), (ws, w_new[k].at[at]), (mo, m_new[k].at[local]), (vo, v_new[k].at[local])]
        outs += [pltpu.make_async_copy(s, d, sem_out.at[j, p]) for p, (s, d) in enumerate(pairs)]
        for c in outs[-4:]:
            c.start()
    for c in outs:
        c.wait()


def adam(idx, layer, own, first, n, mine, theirs, w, m, v, bufs, after=()):
    kinds = 3 if own else 2
    quarter, d = m[0].shape[1], w[0].shape[1]
    ins = [*mine, *theirs, *w[:kinds], *m[:kinds], *v[:kinds]]
    flat = [b[k] for b in bufs for k in range(kinds)] if bufs else []
    shapes = [jax.ShapeDtypeStruct(a.shape, a.dtype) for group in (w, m, v) for a in group[:kinds]]
    shapes += [jax.ShapeDtypeStruct(g.shape, BF) for g in mine]
    scratch = [pltpu.VMEM((4, quarter, n * LN), e) for e in (BF, BF, BF, F32, F32, F32, F32)]
    if own:
        scratch += [pltpu.VMEM((n * LN, d), e) for e in (BF, BF, BF, F32, F32, F32, F32)]
    scratch += [pltpu.SemaphoreType.DMA((5, 5)), pltpu.SemaphoreType.DMA((5, 4))]
    size = sum(g.size for g in mine)
    res = call(
        functools.partial(adam_body, layer, own, first, n, len(flat)),
        idx,
        (1,),
        [None] * (len(ins) + len(flat)),
        [(None, s) for s in shapes],
        ins + flat,
        scratch=scratch,
        aliases={len(ins) + j: j for j in range(len(flat))},
        nbytes=26 * size,
        after=after,
    )
    return [list(res[kinds * j : kinds * j + kinds]) for j in range(3)], res[3 * kinds :]


def place_body(layer, own, first, n, quarter, idx, *refs):
    kinds = 3 if own else 2
    each = kinds - 1
    pieces, rest = refs[: 3 * each], refs[3 * each + kinds :]
    outs, scratch, (sem_in, sem_out) = rest[:kinds], rest[kinds:-2], rest[-2:]
    xi, ci = idx[0], idx[1]
    part = outs[0].shape[2] // 4
    into = [pltpu.make_async_copy(p, s, sem_in.at[j]) for j, (p, s) in enumerate(zip(pieces, scratch))]
    for c in into:
        c.start()
    done = []
    for j, (px, pc) in enumerate(((xi, 1 - ci), (1 - xi, ci), (1 - xi, 1 - ci))):
        gu, down = places(layer, own, first, n, quarter, part, px, pc)
        into[each * j].wait()
        todo = [(scratch[each * j].at[g], outs[k].at[at]) for g, (k, at) in enumerate(gu)]
        if own:
            into[each * j + 1].wait()
            todo.append((scratch[each * j + 1], outs[2].at[down]))
        for p, (s, d) in enumerate(todo):
            done.append(pltpu.make_async_copy(s, d, sem_out.at[j, p]))
            done[-1].start()
    for c in done:
        c.wait()


def place(idx, layer, own, first, n, pieces, w_new, after=()):
    kinds = 3 if own else 2
    flat = [p for one in pieces for p in one]
    return call(
        functools.partial(place_body, layer, own, first, n, pieces[0][0].shape[1]),
        idx,
        (1,),
        [None] * (len(flat) + kinds),
        [(None, jax.ShapeDtypeStruct(a.shape, a.dtype)) for a in w_new[:kinds]],
        flat + list(w_new[:kinds]),
        scratch=[pltpu.VMEM(p.shape, BF) for p in flat] + [pltpu.SemaphoreType.DMA((6,)), pltpu.SemaphoreType.DMA((3, 5))],
        aliases={len(flat) + k: k for k in range(kinds)},
        nbytes=sum(p.size * 4 for p in flat),
        after=after,
    )


def solution(mesh):
    core = [(0, 1), (1, 0), (2, 3), (3, 2)]
    cross = [(0, 2), (2, 0), (1, 3), (3, 1)]
    to_core = lambda ts: [lax.ppermute(t, "dp", core) for t in ts]
    to_cross = lambda ts: [lax.ppermute(t, "dp", cross) for t in ts]

    def step(x, dy, *arrays):
        w, m, v = arrays[:3], arrays[3:6], arrays[6:]
        me = lax.axis_index("dp")
        idx = jnp.stack([me // 2, me % 2]).astype(jnp.int32)
        x, dy = x[0], dy[0]
        t, d = x.shape
        n = w[0].shape[2] // 4 // LN
        mine = lambda s, q, k=0: (2 * s[0] + q) * n + k
        other = lambda s, q, k=0: (2 * (1 - s[0]) + q) * n + k
        after = lambda base, k: lambda s, q: base(s, q) + k

        (x_far,) = to_cross([x])
        (dy_far,) = to_cross([dy])
        near = forward(idx, x, w, 2 * t, 0, 512, ())
        a1, a1_t = near[4], near[5]
        *parts, da_near = middle(idx, 0, a1, a1_t, [dy], w, n, mine, parts_out=True)
        gate, up, h1, a0_t, a1, a1_t = forward(idx, x_far, w, 2 * t, t, 512, near, after=[da_near])
        *grads, da_far = middle(idx, 1, a1, a1_t, [dy_far], w, n, mine, parts=parts)

        bufs = None

        def update(layer, own, first, count, grads, after=()):
            nonlocal bufs
            got = to_core(grads[1::2])
            new, pieces = adam(idx, layer, own, first, count, grads[0::2], got, w, m, v, bufs, after)
            bufs = [list(a) + (list(b[2:]) if bufs and not own else []) for a, b in zip(new, bufs or new)]
            far = to_cross(pieces)
            return pieces, (layer, own, first, count, [to_core(pieces), far, to_core(far)])

        def put(job, after=()):
            layer, own, first, count, pieces = job
            got = place(idx, layer, own, first, count, pieces, bufs[0], after)
            bufs[0][: len(got)] = got

        pieces, job_a = update(1, True, 0, n, grads)
        *grads, dh1 = middle(idx, 0, a1, a1_t, [dy, dy_far], w, n, other, das=(da_near, da_far), h1=h1, after=pieces)
        pieces, job_b = update(1, False, 0, n, grads)
        grads = backward(idx, dh1, a0_t, gate, up, w[2], OWN0, mine, True, after=pieces)
        pieces, job_c = update(0, True, 0, OWN0, grads)
        grads = backward(idx, dh1, a0_t, gate, up, w[2], n - OWN0, after(mine, OWN0), True, after=pieces)
        pieces, job_d = update(0, True, OWN0, n - OWN0, grads)
        grads = backward(idx, dh1, a0_t, gate, up, w[2], n, other, False, after=pieces)
        pieces, job_e = update(0, False, 0, n, grads)
        for job in (job_a, job_b, job_c, job_d, job_e):
            put(job, pieces)
        return tuple(bufs[j][k] for j in range(3) for k in range(3))

    tok, rep, mom = P(("rep", "dp")), P(), P(None, "dp")
    return jax.shard_map(
        step,
        mesh=mesh,
        in_specs=(tok, tok, rep, rep, rep) + (mom,) * 6,
        out_specs=(P("rep"),) * 3 + (P("rep", "dp"),) * 6,
        check_vma=False,
    )
```
